32 devices in a mesh: bits: 32 (over z, y, x, core).
Axes of the slice: x: 2, y: 2, z: 4, core: 2. Of those that a mesh axis runs over, the one named last changes fastest.
Arguments:
- environment: float32 [2, 128, 64, 4096], P(None, 'bits'), may hold values from -6 to 6
- peps: float32 [2, 2, 8, 8, 8, 8], replicated, may hold values from -2 to 2
- operators: float32 [2, 2, 2], replicated, may hold values from -4 to 4
- gauge: float32 [128, 128], replicated, may hold values from -0.5 to 0.5
Outputs:
- absorbed: float32 [2, 128, 262144], P(None, None, 'bits')
- rms: float32 [2], replicated
The draws below stay inside these ranges and needn't reach their ends.
All inputs are finite; a program needn't handle non-finite values.
Results may differ from the reference program's by a relative error of at most 0.0003.
Values sent between devices are 32-bit elements; how exact they have to be, the bound alone decides.
A program may use at most 512 MiB of HBM per device.

```python
import jax
import jax.numpy as jnp
from jax import lax

D = 8
PHYS = 2
CHI = 128
COLS = 2
NENV = 2
LEGS = 4096


def draw_peps(key, part):
    first, second = jax.random.split(jax.random.fold_in(key, 17), 2)
    shape = (COLS, PHYS, D, D, D, D)
    base = jax.random.truncated_normal(first, -4.0, 4.0, shape, jnp.float32)
    ramp = 3.0 ** (jnp.arange(D, dtype=jnp.float32) / (D - 1))
    rough = jnp.exp(jax.random.uniform(second, (COLS, 1, 1, 1, 1, D), jnp.float32, -0.2, 0.2))
    return (base / D * ramp * rough).astype(jnp.float32)


def levels(own_key, dims, shards, low, largest):
    loudness = 1.0
    for axis_at, parts in shards:
        draws = jax.random.uniform(jax.random.fold_in(jax.random.fold_in(own_key, 6), axis_at), (parts,), jnp.float32, low / len(shards), largest / len(shards))
        loudness = loudness * jnp.repeat(jnp.exp(draws), dims[axis_at] // parts).reshape((-1,) + (1,) * (len(dims) - 1 - axis_at))
    return loudness


def noise(stream_key, dims, spread, most, pieces=(), kind=jnp.bfloat16):
    entries = spread * jax.random.normal(stream_key, dims, jnp.float32)
    if pieces:
        entries = entries * levels(stream_key, dims, pieces, -0.22, 0.18)
    return jnp.clip(entries, -most, most).astype(kind)


def setup_inputs(seed: int = 0) -> dict:
    streams_of = jax.random.split(jax.random.key(seed), 5)
    environment = noise(streams_of[0], (NENV, CHI, D * D, LEGS), 1.0, 6.0, ((1, 32),), jnp.float32)
    peps = draw_peps(jax.random.fold_in(streams_of[4], 71), 0)
    operators = noise(streams_of[2], (COLS, PHYS, PHYS), 1.0, 4.0, (), jnp.float32)
    gauge = noise(streams_of[3], (CHI, CHI), CHI ** -0.5, 0.5, (), jnp.float32)
    return {"environment": environment, "peps": peps, "operators": operators, "gauge": gauge}


EPS = 1e-06

def absorb(state, peps, operators):
    count, rows = (state.shape[0], state.shape[1])
    width = peps.shape[2]
    columns = peps.shape[0]
    for column in range(columns):
        before = width ** (2 * column)
        after = width ** (2 * (columns - 1 - column))
        view = state.reshape(count, rows, width, width, before, width, width, after)
        bra_side = jnp.einsum('pq,qbvms->pbvms', operators[column], peps[column], precision=lax.Precision.HIGHEST)
        partial_value = jnp.einsum('eclbzuvx,plukr->ecrpbzkvx', view, peps[column], precision=lax.Precision.HIGHEST)
        state = jnp.einsum('ecrpbzkvx,pbvms->ecrszkmx', partial_value, bra_side, precision=lax.Precision.HIGHEST)
    return state.reshape(count, rows, -1)

def reference(environment, peps, operators, gauge):

    def single(block):
        grown = absorb(block[None], peps, operators)[0]
        return jnp.dot(gauge, grown, precision=lax.Precision.HIGHEST, preferred_element_type=jnp.float32)
    gauged = lax.map(single, environment)
    mean = lax.optimization_barrier(jnp.mean(gauged * gauged, axis=(1, 2)))
    absorbed = gauged * lax.rsqrt(mean + EPS)[:, None, None]
    return (absorbed, jnp.sqrt(mean))
```

```python
import functools

import jax
import jax.numpy as jnp
from jax import lax
from jax.experimental import pallas as pl
from jax.experimental.pallas import tpu as pltpu
from jax.sharding import PartitionSpec as P

EPS = 1e-06
LANES = 128
SUBLANES = 8
PITCH_PAD = 8
MESH = pl.DeviceIdType.MESH


def rows_of(start, size, stride=None, align=SUBLANES):
    if stride is None:
        return pl.ds(pl.multiple_of(start, align), size)
    return pl.ds(start, size, stride=stride)


def split_parts(value):
    high = value.astype(jnp.bfloat16)
    low = (value - high.astype(jnp.float32)).astype(jnp.bfloat16)
    return high, low


def product(weights, value):
    high, low = split_parts(value)
    return jnp.dot(weights, jnp.concatenate([high, high, low], axis=0), preferred_element_type=jnp.float32)


def exchange_halves(first, second):
    half = LANES // 2
    lower = lax.broadcasted_iota(jnp.int32, first.shape, 1) < half
    return (
        jnp.where(lower, first, pltpu.roll(second, half, 1)),
        jnp.where(lower, pltpu.roll(first, half, 1), second),
    )


def flipped(index, other, n):
    total, bit = 0, 1
    while bit < n:
        total = total + ((index // bit + other // bit) % 2) * bit
        bit *= 2
    return total


def prepare_weights(w, peps, operators, gauge, turn, kets, bras, gauge_parts):
    square = w * w
    blocks = []
    for j in range(2):
        blocks.append(jnp.concatenate([
            peps[2 * j + p, pl.ds(d, square, stride=w), :] for p in range(2) for d in range(w)
        ], axis=1))
    turn[0] = jnp.concatenate(blocks, axis=0).T
    layers = []
    for p in range(2):
        layers.append(jnp.concatenate([turn[0, pl.ds(p * square + r, w, stride=w), :] for r in range(w)], axis=0))

    def halves(value):
        high, low = split_parts(value)
        return high.astype(jnp.float32), low.astype(jnp.float32)

    high, low = halves(jnp.concatenate(layers, axis=0))
    for j, (first, third) in enumerate(zip(exchange_halves(high, low), (high, pltpu.roll(high, LANES // 2, 1)))):
        kets[j, :, :LANES] = first.astype(jnp.bfloat16)
        kets[j, :, LANES:] = third[:, :square].astype(jnp.bfloat16)
    mixed = [[operators[j, p, 0] * layers[0] + operators[j, p, 1] * layers[1] for p in range(2)] for j in range(2)]
    for j in range(2):
        high, low = split_parts(exchange_halves(*mixed[j])[j])
        for at, part in enumerate((high, low, high)):
            bras[j, :, at * LANES:(at + 1) * LANES] = part
    high, low = split_parts(gauge[...])
    for at, part in enumerate((high, low, high)):
        chi = high.shape[1]
        gauge_parts[:, at * chi:(at + 1) * chi] = part


def absorb_group(w, t, source, wide, middle, turn, kets, bras, outgoing, order, finished):
    square = w * w
    pitch = 2 * square + PITCH_PAD
    pieces = source.shape[0] // w // outgoing.shape[0]
    half = w // 2
    per_bond = outgoing.shape[1] // square

    def fill(block, value):
        wide[rows_of(block * pitch, 2 * square), :] = value

    def first(bond, carry):
        columns = []
        for piece in range(pieces):
            columns += exchange_halves(*[
                source[pl.ds(((t + low) * pieces + piece) * w, w), pl.ds(bond, w, stride=w), :].reshape(square, LANES)
                for low in range(2)
            ])
        result = product(kets[0], jnp.concatenate(columns, axis=1))
        for at in range(w):
            fill(bond * w + at, result[:, at * LANES:(at + 1) * LANES])
        return carry

    def turned(bra, bond):
        columns = []
        for leg in range(w):
            columns.append(jnp.concatenate([
                wide[pl.ds(p * square + bond * w + leg, square, stride=pitch), :] for p in range(2)
            ], axis=0))
        result = product(bra, jnp.concatenate(columns, axis=1))
        for pair in range(half):
            yield pair, jnp.concatenate([
                result[out * w:(out + 1) * w, leg * LANES:(leg + 1) * LANES]
                for out in (2 * pair, 2 * pair + 1) for leg in range(w)
            ], axis=0).T

    def second(bond, carry):
        for pair, block in turned(bras[0], bond):
            middle[rows_of((bond * half + pair) * LANES, LANES), :] = block
        return carry

    def third(pair, carry):
        columns = [[], []]
        for leg in range(w):
            values = exchange_halves(*[
                jnp.concatenate([
                    middle[pl.ds((other * half + pair) * LANES + low * square + leg, w, stride=w), :]
                    for other in range(w)
                ], axis=0)
                for low in range(2)
            ])
            for low in range(2):
                columns[low].append(values[low])
        result = product(kets[1], jnp.concatenate(columns[0] + columns[1], axis=1))
        for at in range(2 * w):
            fill(pair * 2 * w + at, result[:, at * LANES:(at + 1) * LANES])
        return carry

    def fourth(step, carry):
        bond = order(step)
        for pair, block in turned(bras[1], bond):
            turn[pair] = block
            even = turn[pair, pl.ds(0, square, stride=2), :]
            odd = turn[pair, pl.ds(1, square, stride=2), :]
            for low, value in enumerate(exchange_halves(even, odd)):
                at = (bond * w + pair * 2 + low) * per_bond
                for row in range(2):
                    outgoing[t + row, rows_of(at, per_bond), :] = value[row * per_bond:(row + 1) * per_bond]

        @pl.when(step > 0)
        def _():
            finished(order(step - 1))

        return carry

    lax.fori_loop(0, w, first, 0)
    lax.fori_loop(0, w, second, 0)
    lax.fori_loop(0, half, third, 0)
    lax.fori_loop(0, w, fourth, 0)
    finished(order(w - 1))


def program_kernel(
    n, w, rows, x_ref, peps_ref, operators, gauge_ref, out_ref, sums_ref,
    source, wide, middle, turn, peps, gauge, kets, bras, gauge_parts, outgoing, incoming, totals, parts,
    load_sem, small_sem, send_sem, whole_sem, chunk_sem, sum_sem,
):
    square = w * w
    entries = outgoing.shape[0]
    count = entries // rows
    share = incoming.shape[2]
    pieces = source.shape[0] // w // entries
    step = w * LANES * pieces // w
    chunk = min(share, SUBLANES)
    me = lax.axis_index("bits")

    barrier = pltpu.get_barrier_semaphore()

    def greet(k, carry):
        pl.semaphore_signal(barrier, inc=1, device_id=((me + k) % n,), device_id_type=MESH)
        return carry

    lax.fori_loop(1, n, greet, 0)

    smalls = [pltpu.make_async_copy(peps_ref, peps, small_sem.at[0]), pltpu.make_async_copy(gauge_ref, gauge, small_sem.at[1])]
    for copy in smalls:
        copy.start()

    def load(group, carry):
        def load_leg(at, carry):
            t = 2 * group + at // w
            leg = at % w
            for piece in range(pieces):
                pltpu.make_async_copy(
                    x_ref.at[t // rows, t % rows, :, :, pl.ds(pl.multiple_of(leg * step + piece * LANES, LANES), LANES)],
                    source.at[pl.ds((t * pieces + piece) * w, w), rows_of(leg * w, w), :],
                    load_sem.at[group],
                ).start()
            return carry

        return lax.fori_loop(0, 2 * w, load_leg, carry)

    lax.fori_loop(0, entries // 2, load, 0)
    for copy in smalls:
        copy.wait()
    prepare_weights(w, peps, operators, gauge, turn, kets, bras, gauge_parts)
    pl.semaphore_wait(barrier, n - 1)

    def send_whole(t, kr):
        def some(k, carry):
            dest = kr * (n // w) + flipped(me % (n // w), k, n // w)

            @pl.when(dest != me)
            def _():
                pltpu.make_async_remote_copy(
                    src_ref=outgoing.at[t, rows_of(dest * share, share), :],
                    dst_ref=incoming.at[0, me * rows + t % rows],
                    send_sem=send_sem.at[0],
                    recv_sem=whole_sem.at[0],
                    device_id=(dest,),
                    device_id_type=MESH,
                ).start()

            return carry

        lax.fori_loop(0, n // w, some, 0)

    def order(at):
        mine = me // (n // w)
        return flipped(mine, flipped(at, w // 2, w), w)

    def group_step(group, carry):
        t = 2 * group
        block = source.at[pl.ds(t * pieces * w, 2 * pieces * w)]
        pltpu.make_async_copy(block, block, load_sem.at[group]).wait()

        def finished(kr):
            for low in range(2):
                @pl.when(t + low < rows)
                def _():
                    send_whole(t + low, kr)

        absorb_group(w, t, source, wide, middle, turn, kets, bras, outgoing, order, finished)
        return carry

    lax.fori_loop(0, entries // 2, group_step, 0)

    def own(t, carry):
        incoming[t // rows, me * rows + t % rows] = outgoing[t, rows_of(me * share, share), :]
        return carry

    lax.fori_loop(0, entries, own, 0)

    for e in range(1, count):
        def send_chunk(q, carry):
            def some(k, carry):
                dest = flipped(me, k // 2 + (k % 2) * (n // 2), n)
                pltpu.make_async_remote_copy(
                    src_ref=outgoing.at[pl.ds(e * rows, rows), rows_of(dest * share + q * chunk, chunk), :],
                    dst_ref=incoming.at[e, pl.ds(me * rows, rows), rows_of(q * chunk, chunk), :],
                    send_sem=send_sem.at[e],
                    recv_sem=chunk_sem.at[e - 1, q],
                    device_id=(dest,),
                    device_id_type=MESH,
                ).start()
                return carry

            return lax.fori_loop(1, n, some, carry)

        lax.fori_loop(0, share // chunk, send_chunk, 0)

    def gauged(e, at, total):
        value = jnp.concatenate([incoming[e, :, at * chunk + i, :] for i in range(chunk)], axis=1)
        result = jnp.dot(
            gauge_parts[...], jnp.concatenate([*split_parts(value)[:1] * 2, split_parts(value)[1]], axis=0),
            preferred_element_type=jnp.float32,
        )
        out_ref[e, :, pl.ds(pl.multiple_of(at * chunk * LANES, LANES), chunk * LANES)] = result
        return total + jnp.sum(result * result, axis=0, keepdims=True)

    half = LANES // count
    folded = []
    for e in range(count):
        if e == 0:
            block = incoming.at[0, pl.ds(0, (n - 1) * rows)]
            pltpu.make_async_copy(block, block, whole_sem.at[0]).wait()

        def some(at, total):
            if e > 0:
                block = incoming.at[e, pl.ds(0, (n - 1) * rows), rows_of(at * chunk, chunk), :]
                pltpu.make_async_copy(block, block, chunk_sem.at[e - 1, at]).wait()
            return gauged(e, at, total)

        total = lax.fori_loop(0, share // chunk, some, jnp.zeros((1, chunk * LANES), jnp.float32))
        total = sum(total[:, i * LANES:(i + 1) * LANES] for i in range(chunk))
        folded.append(sum(pltpu.roll(total, i * half, 1) for i in range(count)))
    lane = lax.broadcasted_iota(jnp.int32, (1, LANES), 1)
    mixed = folded[0]
    for e in range(1, count):
        mixed = jnp.where(lane // half == e, folded[e], mixed)
    parts[...] = jnp.broadcast_to(mixed, parts.shape)
    totals[me] = parts[...]

    for e in range(count):
        sent = outgoing.at[pl.ds(0, rows), pl.ds(0, (n - 1) * share)]
        pltpu.make_async_copy(sent, sent, send_sem.at[e]).wait()

    def tell(k, carry):
        pltpu.make_async_remote_copy(
            src_ref=parts.at[pl.ds(0, 1)],
            dst_ref=totals.at[me, pl.ds(0, 1)],
            send_sem=sum_sem.at[0],
            recv_sem=sum_sem.at[1],
            device_id=((me + k) % n,),
            device_id_type=MESH,
        ).start()
        return carry

    lax.fori_loop(1, n, tell, 0)
    heard = totals.at[pl.ds(0, n - 1), pl.ds(0, 1)]
    for at in (1, 0):
        pltpu.make_async_copy(heard, heard, sum_sem.at[at]).wait()
    total = jnp.sum(totals[:, 0, :], axis=0, keepdims=True)
    for e in range(count):
        value = jnp.sum(jnp.where(lane // half == e, total, 0.0), axis=1, keepdims=True)
        sums_ref[e:e + 1, :] = jnp.broadcast_to(value, (1, LANES))


def body(environment, peps, operators, gauge):
    count, rows, square, legs = environment.shape
    n = lax.axis_size("bits")
    w = peps.shape[2]
    chi = rows * n
    entries = count * rows
    lines = square * legs // LANES
    share = lines // n
    chunk = min(share, SUBLANES)
    pieces = legs // w // LANES
    hbm = pl.BlockSpec(memory_space=pltpu.HBM)
    vmem = pl.BlockSpec(memory_space=pltpu.VMEM)
    gauged, sums = pl.pallas_call(
        functools.partial(program_kernel, n, w, rows),
        out_shape=(
            jax.ShapeDtypeStruct((count, chi, share * LANES), jnp.float32),
            jax.ShapeDtypeStruct((SUBLANES, LANES), jnp.float32),
        ),
        in_specs=[hbm, hbm, pl.BlockSpec(memory_space=pltpu.SMEM), hbm],
        out_specs=(vmem, vmem),
        scratch_shapes=[
            pltpu.VMEM((entries * pieces * w, square, LANES), jnp.float32),
            pltpu.VMEM((square * (2 * square + PITCH_PAD), LANES), jnp.float32),
            pltpu.VMEM((square // 2 * LANES, LANES), jnp.float32),
            pltpu.VMEM((w // 2, LANES, LANES), jnp.float32),
            pltpu.VMEM((4, w ** 3, w), jnp.float32),
            pltpu.VMEM((chi, chi), jnp.float32),
            pltpu.VMEM((2, 2 * square, 3 * square), jnp.bfloat16),
            pltpu.VMEM((2, square, 6 * square), jnp.bfloat16),
            pltpu.VMEM((chi, 3 * chi), jnp.bfloat16),
            pltpu.VMEM((entries, lines, LANES), jnp.float32),
            pltpu.VMEM((count, chi, share, LANES), jnp.float32),
            pltpu.VMEM((n, SUBLANES, LANES), jnp.float32),
            pltpu.VMEM((SUBLANES, LANES), jnp.float32),
            pltpu.SemaphoreType.DMA((entries // 2,)),
            pltpu.SemaphoreType.DMA((2,)),
            pltpu.SemaphoreType.DMA((count,)),
            pltpu.SemaphoreType.DMA((1,)),
            pltpu.SemaphoreType.DMA((max(count - 1, 1), share // chunk)),
            pltpu.SemaphoreType.DMA((2,)),
        ],
        compiler_params=pltpu.CompilerParams(
            collective_id=0, has_side_effects=True, vmem_limit_bytes=52 * 1024 * 1024
        ),
        name="absorb_exchange_gauge",
    )(
        environment.reshape(count, rows, w, w, legs),
        peps.reshape(4, w ** 3, w),
        operators,
        gauge,
    )
    mean = sums[:count, 0] / (chi * square * legs)
    scale = lax.rsqrt(mean + EPS)
    return (gauged * scale[:, None, None], jnp.sqrt(mean))


def solution(mesh):
    placed = (P(None, "bits", None, None), P(), P(), P())
    return jax.shard_map(
        body, mesh=mesh, in_specs=placed, out_specs=(P(None, None, "bits"), P()), check_vma=False
    )
```

```python
import functools

import jax
import jax.numpy as jnp
from jax import lax
from jax.experimental import pallas as pl
from jax.experimental.pallas import tpu as pltpu
from jax.sharding import PartitionSpec as P

EPS = 1e-06
LANES = 128
SUBLANES = 8
PITCH_PAD = 8
MESH = pl.DeviceIdType.MESH


def rows_of(start, size, stride=None, align=SUBLANES):
    if stride is None:
        return pl.ds(pl.multiple_of(start, align), size)
    return pl.ds(start, size, stride=stride)


def split_parts(value):
    high = value.astype(jnp.bfloat16)
    low = (value - high.astype(jnp.float32)).astype(jnp.bfloat16)
    return high, low


def product(weights, value):
    high, low = split_parts(value)
    return jnp.dot(weights, jnp.concatenate([high, high, low], axis=0), preferred_element_type=jnp.float32)


def exchange_halves(first, second):
    half = LANES // 2
    lower = lax.broadcasted_iota(jnp.int32, first.shape, 1) < half
    return (
        jnp.where(lower, first, pltpu.roll(second, half, 1)),
        jnp.where(lower, pltpu.roll(first, half, 1), second),
    )


def flipped(index, other, n):
    total, bit = 0, 1
    while bit < n:
        total = total + ((index // bit + other // bit) % 2) * bit
        bit *= 2
    return total


def prepare_weights(w, peps, operators, gauge, turn, kets, bras, gauge_parts):
    square = w * w
    blocks = []
    for j in range(2):
        blocks.append(jnp.concatenate([
            peps[2 * j + p, pl.ds(d, square, stride=w), :] for p in range(2) for d in range(w)
        ], axis=1))
    turn[0] = jnp.concatenate(blocks, axis=0).T
    layers = []
    for p in range(2):
        layers.append(jnp.concatenate([turn[0, pl.ds(p * square + r, w, stride=w), :] for r in range(w)], axis=0))

    def halves(value):
        high, low = split_parts(value)
        return high.astype(jnp.float32), low.astype(jnp.float32)

    high, low = halves(jnp.concatenate(layers, axis=0))
    for j, (first, third) in enumerate(zip(exchange_halves(high, low), (high, pltpu.roll(high, LANES // 2, 1)))):
        kets[j, :, :LANES] = first.astype(jnp.bfloat16)
        kets[j, :, LANES:] = third[:, :square].astype(jnp.bfloat16)
    mixed = [
        [sum(operators[j, p:p + 1, q:q + 1] * layers[q] for q in range(2)) for p in range(2)] for j in range(2)
    ]
    for j in range(2):
        high, low = split_parts(exchange_halves(*mixed[j])[j])
        for at, part in enumerate((high, low, high)):
            bras[j, :, at * LANES:(at + 1) * LANES] = part
    high, low = split_parts(gauge[...])
    for at, part in enumerate((high, low, high)):
        chi = high.shape[1]
        gauge_parts[:, at * chi:(at + 1) * chi] = part


def absorb_group(w, t, source, wide, middle, turn, kets, bras, outgoing, order):
    square = w * w
    pitch = 2 * square + PITCH_PAD
    pieces = source.shape[0] // w // outgoing.shape[0]
    half = w // 2
    per_bond = outgoing.shape[1] // square

    def fill(block, value):
        wide[rows_of(block * pitch, 2 * square), :] = value

    def first(bond, carry):
        columns = []
        for piece in range(pieces):
            columns += exchange_halves(*[
                source[pl.ds(((t + low) * pieces + piece) * w, w), pl.ds(bond, w, stride=w), :].reshape(square, LANES)
                for low in range(2)
            ])
        result = product(kets[0], jnp.concatenate(columns, axis=1))
        for at in range(w):
            fill(bond * w + at, result[:, at * LANES:(at + 1) * LANES])
        return carry

    def turned(bra, bond):
        columns = []
        for leg in range(w):
            columns.append(jnp.concatenate([
                wide[pl.ds(p * square + bond * w + leg, square, stride=pitch), :] for p in range(2)
            ], axis=0))
        result = product(bra, jnp.concatenate(columns, axis=1))
        for pair in range(half):
            yield pair, jnp.concatenate([
                result[out * w:(out + 1) * w, leg * LANES:(leg + 1) * LANES]
                for out in (2 * pair, 2 * pair + 1) for leg in range(w)
            ], axis=0).T

    def second(bond, carry):
        for pair, block in turned(bras[0], bond):
            middle[rows_of((bond * half + pair) * LANES, LANES), :] = block
        return carry

    def third(pair, carry):
        columns = [[], []]
        for leg in range(w):
            values = exchange_halves(*[
                jnp.concatenate([
                    middle[pl.ds((other * half + pair) * LANES + low * square + leg, w, stride=w), :]
                    for other in range(w)
                ], axis=0)
                for low in range(2)
            ])
            for low in range(2):
                columns[low].append(values[low])
        result = product(kets[1], jnp.concatenate(columns[0] + columns[1], axis=1))
        for at in range(2 * w):
            fill(pair * 2 * w + at, result[:, at * LANES:(at + 1) * LANES])
        return carry

    def fourth(step, carry):
        bond = order(step)
        for pair, block in turned(bras[1], bond):
            turn[pair] = block
            even = turn[pair, pl.ds(0, square, stride=2), :]
            odd = turn[pair, pl.ds(1, square, stride=2), :]
            for low, value in enumerate(exchange_halves(even, odd)):
                at = (bond * w + pair * 2 + low) * per_bond
                for row in range(2):
                    outgoing[t + row, rows_of(at, per_bond), :] = value[row * per_bond:(row + 1) * per_bond]

        return carry

    lax.fori_loop(0, w, first, 0, unroll=8)
    lax.fori_loop(0, w, second, 0, unroll=8)
    lax.fori_loop(0, half, third, 0, unroll=4)
    lax.fori_loop(0, w, fourth, 0, unroll=8)


def program_kernel(
    n, w, rows, x_ref, peps_ref, operators_ref, gauge_ref, out_ref, sums_ref,
    source, wide, middle, turn, peps, operators, gauge, kets, bras, gauge_parts, outgoing, incoming, totals, parts,
    load_sem, small_sem, send_sem, whole_sem, chunk_sem, sum_sem,
):
    square = w * w
    entries = outgoing.shape[0]
    count = entries // rows
    share = incoming.shape[2]
    pieces = source.shape[0] // w // entries
    step = w * LANES * pieces // w
    chunk = min(share, SUBLANES)
    me = lax.axis_index("bits")

    barrier = pltpu.get_barrier_semaphore()

    smalls = [
        pltpu.make_async_copy(source_ref, target, small_sem.at[at])
        for at, (source_ref, target) in enumerate(
            ((peps_ref, peps), (operators_ref, operators), (gauge_ref, gauge))
        )
    ]
    for copy in smalls:
        copy.start()

    def load(group):
        for low in range(2):
            t = 2 * group + low
            e, row = t // rows, t % rows
            for leg in range(w):
                for piece in range(pieces):
                    pltpu.make_async_copy(
                        x_ref.at[e, row, :, :, pl.ds(leg * step + piece * LANES, LANES)],
                        source.at[pl.ds((t * pieces + piece) * w, w), pl.ds(leg * w, w), :],
                        load_sem.at[group],
                    ).start()

    load(0)

    def greet(k, carry):
        pl.semaphore_signal(barrier, inc=1, device_id=((me + k) % n,), device_id_type=MESH)
        return carry

    lax.fori_loop(1, n, greet, 0)
    for copy in smalls:
        copy.wait()
    prepare_weights(w, peps, operators, gauge, turn, kets, bras, gauge_parts)

    def send_whole(t):
        def some(k, carry):
            dest = flipped(me, k // 2 + (k % 2) * (n // 2), n)
            pltpu.make_async_remote_copy(
                src_ref=outgoing.at[t, rows_of(dest * share, share), :],
                dst_ref=incoming.at[0, me * rows + t % rows],
                send_sem=send_sem.at[0],
                recv_sem=whole_sem.at[0],
                device_id=(dest,),
                device_id_type=MESH,
            ).start()
            return carry

        lax.fori_loop(1, n, some, 0)

    def order(at):
        return flipped(me // (n // w), flipped(at, w // 2, w), w)

    def group_step(group, carry):
        t = 2 * group
        block = source.at[pl.ds(t * pieces * w, 2 * pieces * w)]
        pltpu.make_async_copy(block, block, load_sem.at[group]).wait()

        @pl.when(group + 1 < entries // 2)
        def _():
            load(group + 1)

        absorb_group(w, t, source, wide, middle, turn, kets, bras, outgoing, order)

        @pl.when(group == 0)
        def _():
            pl.semaphore_wait(barrier, n - 1)

        for low in range(2):
            @pl.when(t + low < rows)
            def _():
                send_whole(t + low)

        return carry

    lax.fori_loop(0, entries // 2, group_step, 0)

    def own(t, carry):
        incoming[t // rows, me * rows + t % rows] = outgoing[t, rows_of(me * share, share), :]
        return carry

    lax.fori_loop(0, entries, own, 0)

    for e in range(1, count):
        def send_chunk(q, carry):
            def some(k, carry):
                dest = flipped(me, k // 2 + (k % 2) * (n // 2), n)
                pltpu.make_async_remote_copy(
                    src_ref=outgoing.at[pl.ds(e * rows, rows), rows_of(dest * share + q * chunk, chunk), :],
                    dst_ref=incoming.at[e, pl.ds(me * rows, rows), rows_of(q * chunk, chunk), :],
                    send_sem=send_sem.at[e],
                    recv_sem=chunk_sem.at[e - 1, q],
                    device_id=(dest,),
                    device_id_type=MESH,
                ).start()
                return carry

            return lax.fori_loop(1, n, some, carry)

        lax.fori_loop(0, share // chunk, send_chunk, 0)

    def gauged(e, at, total):
        value = jnp.concatenate([incoming[e, :, at * chunk + i, :] for i in range(chunk)], axis=1)
        result = jnp.dot(
            gauge_parts[...], jnp.concatenate([*split_parts(value)[:1] * 2, split_parts(value)[1]], axis=0),
            preferred_element_type=jnp.float32,
        )
        out_ref[e, :, pl.ds(pl.multiple_of(at * chunk * LANES, LANES), chunk * LANES)] = result
        return total + jnp.sum(result * result, axis=0, keepdims=True)

    half = LANES // count
    folded = []
    for e in range(count):
        if e == 0:
            block = incoming.at[0, pl.ds(0, (n - 1) * rows)]
            pltpu.make_async_copy(block, block, whole_sem.at[0]).wait()

        def some(at, total):
            if e > 0:
                block = incoming.at[e, pl.ds(0, (n - 1) * rows), rows_of(at * chunk, chunk), :]
                pltpu.make_async_copy(block, block, chunk_sem.at[e - 1, at]).wait()
            return gauged(e, at, total)

        total = lax.fori_loop(0, share // chunk, some, jnp.zeros((1, chunk * LANES), jnp.float32))
        total = sum(total[:, i * LANES:(i + 1) * LANES] for i in range(chunk))
        folded.append(sum(pltpu.roll(total, i * half, 1) for i in range(count)))
    lane = lax.broadcasted_iota(jnp.int32, (1, LANES), 1)
    mixed = folded[0]
    for e in range(1, count):
        mixed = jnp.where(lane // half == e, folded[e], mixed)
    parts[...] = jnp.broadcast_to(mixed, parts.shape)
    totals[me] = parts[...]

    for e in range(count):
        sent = outgoing.at[pl.ds(0, rows), pl.ds(0, (n - 1) * share)]
        pltpu.make_async_copy(sent, sent, send_sem.at[e]).wait()

    def tell(k, carry):
        pltpu.make_async_remote_copy(
            src_ref=parts.at[pl.ds(0, 1)],
            dst_ref=totals.at[me, pl.ds(0, 1)],
            send_sem=sum_sem.at[0],
            recv_sem=sum_sem.at[1],
            device_id=((me + k) % n,),
            device_id_type=MESH,
        ).start()
        return carry

    lax.fori_loop(1, n, tell, 0)
    heard = totals.at[pl.ds(0, n - 1), pl.ds(0, 1)]
    for at in (1, 0):
        pltpu.make_async_copy(heard, heard, sum_sem.at[at]).wait()
    total = jnp.sum(totals[:, 0, :], axis=0, keepdims=True)
    for e in range(count):
        value = jnp.sum(jnp.where(lane // half == e, total, 0.0), axis=1, keepdims=True)
        sums_ref[e:e + 1, :] = jnp.broadcast_to(value, (1, LANES))


def scale_kernel(numel, gauged, sums, out_ref, rms_ref, staged, sems):
    count, chi, width = gauged.shape
    mean = sums[...] * (1.0 / numel)
    lane = lax.broadcasted_iota(jnp.int32, (1, LANES), 1)
    root = jnp.zeros((1, LANES), jnp.float32)
    for e in range(count):
        root = jnp.where(lane == e, jnp.sqrt(mean[e:e + 1, :]), root)
    rms_ref[...] = root.reshape(LANES)[:count]
    blocks = sems.shape[0] // count
    lines = chi // blocks

    def copy(e, at):
        rows = rows_of(at * lines, lines)
        return pltpu.make_async_copy(staged.at[e, rows, :], out_ref.at[e, rows, :], sems.at[e * blocks + at])

    for e in range(count):
        scale = lax.rsqrt(mean[e:e + 1, :1] + EPS)

        def some(at, carry):
            rows = rows_of(at * lines, lines)
            staged[e, rows, :] = gauged[e, rows, :] * scale

            @pl.when(at > 0)
            def _():
                copy(e, at - 1).start()

            if e > 0:
                @pl.when(at == 0)
                def _():
                    copy(e - 1, blocks - 1).start()

            return carry

        lax.fori_loop(0, blocks, some, 0)
    copy(count - 1, blocks - 1).start()
    for e in range(count):
        lax.fori_loop(0, blocks, lambda at, carry: (copy(e, at).wait(), carry)[1], 0)


def scaled(gauged, sums, numel):
    count, chi, width = gauged.shape
    blocks = chi // SUBLANES
    vmem = pl.BlockSpec(memory_space=pltpu.VMEM)
    return pl.pallas_call(
        functools.partial(scale_kernel, numel),
        out_shape=(
            jax.ShapeDtypeStruct(gauged.shape, jnp.float32),
            jax.ShapeDtypeStruct((count,), jnp.float32),
        ),
        in_specs=[vmem, vmem],
        out_specs=(pl.BlockSpec(memory_space=pltpu.HBM), vmem),
        scratch_shapes=[
            pltpu.VMEM(gauged.shape, jnp.float32),
            pltpu.SemaphoreType.DMA((count * blocks,)),
        ],
        compiler_params=pltpu.CompilerParams(vmem_limit_bytes=16 * 1024 * 1024),
        name="scale",
    )(gauged, sums)


def body(environment, peps, operators, gauge):
    count, rows, square, legs = environment.shape
    n = lax.axis_size("bits")
    w = peps.shape[2]
    chi = rows * n
    entries = count * rows
    lines = square * legs // LANES
    share = lines // n
    chunk = min(share, SUBLANES)
    pieces = legs // w // LANES
    hbm = pl.BlockSpec(memory_space=pltpu.HBM)
    vmem = pl.BlockSpec(memory_space=pltpu.VMEM)
    gauged, sums = pl.pallas_call(
        functools.partial(program_kernel, n, w, rows),
        out_shape=(
            jax.ShapeDtypeStruct((count, chi, share * LANES), jnp.float32),
            jax.ShapeDtypeStruct((SUBLANES, LANES), jnp.float32),
        ),
        in_specs=[hbm] * 4,
        out_specs=(vmem, vmem),
        scratch_shapes=[
            pltpu.VMEM((entries * pieces * w, square, LANES), jnp.float32),
            pltpu.VMEM((square * (2 * square + PITCH_PAD), LANES), jnp.float32),
            pltpu.VMEM((square // 2 * LANES, LANES), jnp.float32),
            pltpu.VMEM((w // 2, LANES, LANES), jnp.float32),
            pltpu.VMEM((4, w ** 3, w), jnp.float32),
            pltpu.VMEM((2, 2, 2), jnp.float32),
            pltpu.VMEM((chi, chi), jnp.float32),
            pltpu.VMEM((2, 2 * square, 3 * square), jnp.bfloat16),
            pltpu.VMEM((2, square, 6 * square), jnp.bfloat16),
            pltpu.VMEM((chi, 3 * chi), jnp.bfloat16),
            pltpu.VMEM((entries, lines, LANES), jnp.float32),
            pltpu.VMEM((count, chi, share, LANES), jnp.float32),
            pltpu.VMEM((n, SUBLANES, LANES), jnp.float32),
            pltpu.VMEM((SUBLANES, LANES), jnp.float32),
            pltpu.SemaphoreType.DMA((entries // 2,)),
            pltpu.SemaphoreType.DMA((3,)),
            pltpu.SemaphoreType.DMA((count,)),
            pltpu.SemaphoreType.DMA((1,)),
            pltpu.SemaphoreType.DMA((max(count - 1, 1), share // chunk)),
            pltpu.SemaphoreType.DMA((2,)),
        ],
        compiler_params=pltpu.CompilerParams(
            collective_id=0, has_side_effects=True, vmem_limit_bytes=36 * 1024 * 1024
        ),
        name="absorb_exchange_gauge",
    )(
        pltpu.with_memory_space_constraint(environment.reshape(count, rows, w, w, legs), pltpu.HBM),
        pltpu.with_memory_space_constraint(peps.reshape(4, w ** 3, w), pltpu.HBM),
        pltpu.with_memory_space_constraint(operators, pltpu.HBM),
        pltpu.with_memory_space_constraint(gauge, pltpu.HBM),
    )
    return scaled(gauged, sums, chi * square * legs)


def solution(mesh):
    placed = (P(None, "bits", None, None), P(), P(), P())
    return jax.shard_map(
        body, mesh=mesh, in_specs=placed, out_specs=(P(None, None, "bits"), P()), check_vma=False
    )
```

```python
import functools

import jax
import jax.numpy as jnp
from jax import lax
from jax.experimental import pallas as pl
from jax.experimental.pallas import tpu as pltpu
from jax.sharding import PartitionSpec as P

EPS = 1e-06
LANES = 128
SUBLANES = 8
PITCH_PAD = 8
MESH = pl.DeviceIdType.MESH


def rows_of(start, size, stride=None, align=SUBLANES):
    if stride is None:
        return pl.ds(pl.multiple_of(start, align), size)
    return pl.ds(start, size, stride=stride)


def split_parts(value):
    high = value.astype(jnp.bfloat16)
    low = (value - high.astype(jnp.float32)).astype(jnp.bfloat16)
    return high, low


def product(weights, value):
    high, low = split_parts(value)
    return jnp.dot(weights, jnp.concatenate([high, high, low], axis=0), preferred_element_type=jnp.float32)


def exchange_halves(first, second):
    half = LANES // 2
    lower = lax.broadcasted_iota(jnp.int32, first.shape, 1) < half
    return (
        jnp.where(lower, first, pltpu.roll(second, half, 1)),
        jnp.where(lower, pltpu.roll(first, half, 1), second),
    )


def flips(index, n):
    terms, bit = {}, 1
    while bit < n:
        terms[bit] = bit - 2 * bit * lax.rem(lax.div(index, bit), 2)
        bit *= 2
    return lambda other: sum((term for bit, term in terms.items() if other & bit), index)


def prepare_weights(w, peps, operators, turn, kets, bras):
    square = w * w
    blocks = []
    for j in range(2):
        blocks.append(jnp.concatenate([
            peps[2 * j + p, pl.ds(d, square, stride=w), :] for p in range(2) for d in range(w)
        ], axis=1))
    turn[0] = jnp.concatenate(blocks, axis=0).T
    layers = []
    for p in range(2):
        layers.append(jnp.concatenate([turn[0, pl.ds(p * square + r, w, stride=w), :] for r in range(w)], axis=0))

    def halves(value):
        high, low = split_parts(value)
        return high.astype(jnp.float32), low.astype(jnp.float32)

    high, low = halves(jnp.concatenate(layers, axis=0))
    for j, (first, third) in enumerate(zip(exchange_halves(high, low), (high, pltpu.roll(high, LANES // 2, 1)))):
        kets[j, :, :LANES] = first.astype(jnp.bfloat16)
        kets[j, :, LANES:] = third[:, :square].astype(jnp.bfloat16)
    mixed = [
        [sum(operators[j, p:p + 1, q:q + 1] * layers[q] for q in range(2)) for p in range(2)] for j in range(2)
    ]
    for j in range(2):
        high, low = split_parts(exchange_halves(*mixed[j])[j])
        for at, part in enumerate((high, low, high)):
            bras[j, :, at * LANES:(at + 1) * LANES] = part


def prepare_gauge(gauge, gauge_parts):
    high, low = split_parts(gauge[...])
    chi = high.shape[1]
    for at, part in enumerate((high, low, high)):
        gauge_parts[:, at * chi:(at + 1) * chi] = part


def absorb_group(w, t, source, wide, middle, turn, kets, bras, outgoing, order, finished):
    square = w * w
    pitch = 2 * square + PITCH_PAD
    pieces = source.shape[0] // w // outgoing.shape[0]
    half = w // 2
    per_bond = outgoing.shape[1] // square

    def fill(block, value):
        wide[rows_of(block * pitch, 2 * square), :] = value

    def first(bond, carry):
        for piece in range(pieces):
            values = exchange_halves(*[
                source[pl.ds(((t + low) * pieces + piece) * w, w), pl.ds(bond, w, stride=w), :].reshape(square, LANES)
                for low in range(2)
            ])
            result = product(kets[0], jnp.concatenate(values, axis=1))
            for low in range(2):
                fill(bond * w + piece * 2 + low, result[:, low * LANES:(low + 1) * LANES])
        return carry

    def turned(bra, bond):
        results = []
        for leg in range(0, w, 2):
            result = product(bra, jnp.concatenate([
                jnp.concatenate([
                    wide[pl.ds(p * square + bond * w + leg + low, square, stride=pitch), :] for p in range(2)
                ], axis=0)
                for low in range(2)
            ], axis=1))
            results += [result[:, :LANES], result[:, LANES:]]
        for pair in range(half):
            yield pair, jnp.concatenate([
                results[leg][out * w:(out + 1) * w] for out in (2 * pair, 2 * pair + 1) for leg in range(w)
            ], axis=0).T

    def second(bond, carry):
        for pair, block in turned(bras[0], bond):
            middle[rows_of((bond * half + pair) * LANES, LANES), :] = block
        return carry

    def third(pair, carry):
        for leg in range(w):
            values = exchange_halves(*[
                jnp.concatenate([
                    middle[pl.ds((other * half + pair) * LANES + low * square + leg, w, stride=w), :]
                    for other in range(w)
                ], axis=0)
                for low in range(2)
            ])
            result = product(kets[1], jnp.concatenate(values, axis=1))
            for low in range(2):
                fill((pair * 2 + low) * w + leg, result[:, low * LANES:(low + 1) * LANES])
        return carry

    def fourth(step, carry):
        bond = order(step)
        for pair, block in turned(bras[1], bond):
            turn[pair] = block
            even = turn[pair, pl.ds(0, square, stride=2), :]
            odd = turn[pair, pl.ds(1, square, stride=2), :]
            for low, value in enumerate(exchange_halves(even, odd)):
                at = (bond * w + pair * 2 + low) * per_bond
                for row in range(2):
                    outgoing[t + row, rows_of(at, per_bond), :] = value[row * per_bond:(row + 1) * per_bond]

        return carry

    lax.fori_loop(0, w, first, 0, unroll=8)
    lax.fori_loop(0, w, second, 0, unroll=8)
    lax.fori_loop(0, half, third, 0, unroll=4)
    for begin, end in ((0, 1), (1, half), (half, w)):
        for at in range(begin, end):
            fourth(at, 0)
        finished(begin, end)


def program_kernel(
    n, w, rows, x_ref, peps_ref, operators_ref, gauge_ref, out_ref, sums_ref,
    source, wide, middle, turn, peps, operators, gauge, kets, bras, gauge_parts, outgoing, incoming, totals, parts,
    load_sem, small_sem, send_sem, whole_sem, chunk_sem, sum_sem,
):
    square = w * w
    entries = outgoing.shape[0]
    count = entries // rows
    share = incoming.shape[2]
    pieces = source.shape[0] // w // entries
    step = w * LANES * pieces // w
    chunk = min(share, SUBLANES)
    me = lax.axis_index("bits")
    other = flips(me, n)
    turns = [k // 2 + (k % 2) * (n // 2) for k in range(1, n)]

    barrier = pltpu.get_barrier_semaphore()

    smalls = [
        pltpu.make_async_copy(source_ref, target, small_sem.at[at])
        for at, (source_ref, target) in enumerate(
            ((peps_ref, peps), (operators_ref, operators), (gauge_ref, gauge))
        )
    ]
    for copy in smalls:
        copy.start()

    def load(group):
        for low in range(2):
            t = 2 * group + low
            e, row = (t // rows, t % rows) if isinstance(t, int) else (lax.div(t, rows), lax.rem(t, rows))
            for leg in range(w):
                for piece in range(pieces):
                    pltpu.make_async_copy(
                        x_ref.at[e, row, :, :, pl.ds(leg * step + piece * LANES, LANES)],
                        source.at[pl.ds((t * pieces + piece) * w, w), pl.ds(leg * w, w), :],
                        load_sem.at[group],
                    ).start()

    load(0)

    for k in range(n - 1, 0, -1):
        pl.semaphore_signal(barrier, inc=1, device_id=(other(k),), device_id_type=MESH)
    for copy in smalls[:2]:
        copy.wait()
    prepare_weights(w, peps, operators, turn, kets, bras)

    def send_whole(t, begin, end):
        for k in range(begin * (n // w), end * (n // w)):
            k = k ^ (n // 2)
            if k == 0:
                continue
            dest = other(k)
            pltpu.make_async_remote_copy(
                src_ref=outgoing.at[t, rows_of(dest * share, share), :],
                dst_ref=incoming.at[0, me * rows + lax.rem(t, rows)],
                send_sem=send_sem.at[0],
                recv_sem=whole_sem.at[0],
                device_id=(dest,),
                device_id_type=MESH,
            ).start()

    bond_of = flips(lax.div(me, n // w), w)

    def order(at):
        return bond_of(at ^ (w // 2))

    def group_step(group, carry):
        t = 2 * group
        block = source.at[pl.ds(t * pieces * w, 2 * pieces * w)]
        pltpu.make_async_copy(block, block, load_sem.at[group]).wait()

        @pl.when(group + 1 < entries // 2)
        def _():
            load(group + 1)

        def finished(begin, end):
            if begin == 0:
                @pl.when(group == 0)
                def _():
                    pl.semaphore_wait(barrier, n - 1)

            for low in range(2):
                @pl.when(t + low < rows)
                def _():
                    send_whole(t + low, begin, end)

        absorb_group(w, t, source, wide, middle, turn, kets, bras, outgoing, order, finished)
        return carry

    lax.fori_loop(0, entries // 2, group_step, 0)

    smalls[2].wait()
    prepare_gauge(gauge, gauge_parts)

    def own(t, carry):
        incoming[lax.div(t, rows), me * rows + lax.rem(t, rows)] = outgoing[t, rows_of(me * share, share), :]
        return carry

    lax.fori_loop(0, entries, own, 0)

    for e in range(1, count):
        def send_chunk(q, carry):
            for k in turns:
                dest = other(k)
                pltpu.make_async_remote_copy(
                    src_ref=outgoing.at[pl.ds(e * rows, rows), rows_of(dest * share + q * chunk, chunk), :],
                    dst_ref=incoming.at[e, pl.ds(me * rows, rows), rows_of(q * chunk, chunk), :],
                    send_sem=send_sem.at[e],
                    recv_sem=chunk_sem.at[e - 1, q],
                    device_id=(dest,),
                    device_id_type=MESH,
                ).start()
            return carry

        lax.fori_loop(0, share // chunk, send_chunk, 0)

    def gauged(e, at, total):
        value = jnp.concatenate([incoming[e, :, at * chunk + i, :] for i in range(chunk)], axis=1)
        result = jnp.dot(
            gauge_parts[...], jnp.concatenate([*split_parts(value)[:1] * 2, split_parts(value)[1]], axis=0),
            preferred_element_type=jnp.float32,
        )
        out_ref[e, :, pl.ds(pl.multiple_of(at * chunk * LANES, LANES), chunk * LANES)] = result
        return total + jnp.sum(result * result, axis=0, keepdims=True)

    half = LANES // count
    folded = []
    for e in range(count):
        if e == 0:
            block = incoming.at[0, pl.ds(0, (n - 1) * rows)]
            pltpu.make_async_copy(block, block, whole_sem.at[0]).wait()

        def some(at, total):
            if e > 0:
                block = incoming.at[e, pl.ds(0, (n - 1) * rows), rows_of(at * chunk, chunk), :]
                pltpu.make_async_copy(block, block, chunk_sem.at[e - 1, at]).wait()
            return gauged(e, at, total)

        total = lax.fori_loop(0, share // chunk, some, jnp.zeros((1, chunk * LANES), jnp.float32))
        total = sum(total[:, i * LANES:(i + 1) * LANES] for i in range(chunk))
        folded.append(sum(pltpu.roll(total, i * half, 1) for i in range(count)))
    lane = lax.broadcasted_iota(jnp.int32, (1, LANES), 1)
    mixed = folded[0]
    for e in range(1, count):
        mixed = jnp.where(lane // half == e, folded[e], mixed)
    parts[...] = jnp.broadcast_to(mixed, parts.shape)
    totals[me] = parts[...]

    for k in range(n - 1, 0, -1):
        pltpu.make_async_remote_copy(
            src_ref=parts.at[pl.ds(0, 1)],
            dst_ref=totals.at[me, pl.ds(0, 1)],
            send_sem=sum_sem.at[0],
            recv_sem=sum_sem.at[1],
            device_id=(other(k),),
            device_id_type=MESH,
        ).start()
    for e in range(count):
        sent = outgoing.at[pl.ds(0, rows), pl.ds(0, (n - 1) * share)]
        pltpu.make_async_copy(sent, sent, send_sem.at[e]).wait()
    heard = totals.at[pl.ds(0, n - 1), pl.ds(0, 1)]
    for at in range(2):
        pltpu.make_async_copy(heard, heard, sum_sem.at[at]).wait()
    total = jnp.sum(totals[:, 0, :], axis=0, keepdims=True)
    for e in range(count):
        value = jnp.sum(jnp.where(lane // half == e, total, 0.0), axis=1, keepdims=True)
        sums_ref[e:e + 1, :] = jnp.broadcast_to(value, (1, LANES))


def scale_kernel(numel, gauged, sums, out_ref, rms_ref, staged, roots, sems, root_sem):
    count, chi, width = gauged.shape
    mean = sums[...] * (1.0 / numel)
    lane = lax.broadcasted_iota(jnp.int32, (1, LANES), 1)
    root = jnp.zeros((1, LANES), jnp.float32)
    for e in range(count):
        root = jnp.where(lane == e, jnp.sqrt(mean[e:e + 1, :]), root)
    roots[...] = root.reshape(LANES)[:count]
    blocks = sems.shape[0] // count
    lines = chi // blocks

    def copy(e, at):
        rows = rows_of(at * lines, lines)
        return pltpu.make_async_copy(staged.at[e, rows, :], out_ref.at[e, rows, :], sems.at[e * blocks + at])

    for e in range(count):
        scale = lax.rsqrt(mean[e:e + 1, :1] + EPS)

        def some(at, carry):
            rows = rows_of(at * lines, lines)
            staged[e, rows, :] = gauged[e, rows, :] * scale

            @pl.when(at > 0)
            def _():
                copy(e, at - 1).start()

            if e > 0:
                @pl.when(at == 0)
                def _():
                    copy(e - 1, blocks - 1).start()

            return carry

        lax.fori_loop(0, blocks, some, 0)
        if e == 0:
            rms = pltpu.make_async_copy(roots, rms_ref, root_sem.at[0])
            rms.start()
    copy(count - 1, blocks - 1).start()
    for e in range(count):
        lax.fori_loop(0, blocks, lambda at, carry: (copy(e, at).wait(), carry)[1], 0)
    rms.wait()


def scaled(gauged, sums, numel):
    count, chi, width = gauged.shape
    blocks = chi // (2 * SUBLANES)
    vmem = pl.BlockSpec(memory_space=pltpu.VMEM)
    return pl.pallas_call(
        functools.partial(scale_kernel, numel),
        out_shape=(
            jax.ShapeDtypeStruct(gauged.shape, jnp.float32),
            jax.ShapeDtypeStruct((count,), jnp.float32),
        ),
        in_specs=[vmem, vmem],
        out_specs=(pl.BlockSpec(memory_space=pltpu.HBM),) * 2,
        scratch_shapes=[
            pltpu.VMEM(gauged.shape, jnp.float32),
            pltpu.VMEM((count,), jnp.float32),
            pltpu.SemaphoreType.DMA((count * blocks,)),
            pltpu.SemaphoreType.DMA((1,)),
        ],
        compiler_params=pltpu.CompilerParams(vmem_limit_bytes=16 * 1024 * 1024),
        name="scale",
    )(gauged, sums)


def body(environment, peps, operators, gauge):
    count, rows, square, legs = environment.shape
    n = lax.axis_size("bits")
    w = peps.shape[2]
    chi = rows * n
    entries = count * rows
    lines = square * legs // LANES
    share = lines // n
    chunk = min(share, SUBLANES)
    pieces = legs // w // LANES
    hbm = pl.BlockSpec(memory_space=pltpu.HBM)
    vmem = pl.BlockSpec(memory_space=pltpu.VMEM)
    gauged, sums = pl.pallas_call(
        functools.partial(program_kernel, n, w, rows),
        out_shape=(
            jax.ShapeDtypeStruct((count, chi, share * LANES), jnp.float32),
            jax.ShapeDtypeStruct((SUBLANES, LANES), jnp.float32),
        ),
        in_specs=[hbm] * 4,
        out_specs=(vmem, vmem),
        scratch_shapes=[
            pltpu.VMEM((entries * pieces * w, square, LANES), jnp.float32),
            pltpu.VMEM((square * (2 * square + PITCH_PAD), LANES), jnp.float32),
            pltpu.VMEM((square // 2 * LANES, LANES), jnp.float32),
            pltpu.VMEM((w // 2, LANES, LANES), jnp.float32),
            pltpu.VMEM((4, w ** 3, w), jnp.float32),
            pltpu.VMEM((2, 2, 2), jnp.float32),
            pltpu.VMEM((chi, chi), jnp.float32),
            pltpu.VMEM((2, 2 * square, 3 * square), jnp.bfloat16),
            pltpu.VMEM((2, square, 6 * square), jnp.bfloat16),
            pltpu.VMEM((chi, 3 * chi), jnp.bfloat16),
            pltpu.VMEM((entries, lines, LANES), jnp.float32),
            pltpu.VMEM((count, chi, share, LANES), jnp.float32),
            pltpu.VMEM((n, SUBLANES, LANES), jnp.float32),
            pltpu.VMEM((SUBLANES, LANES), jnp.float32),
            pltpu.SemaphoreType.DMA((entries // 2,)),
            pltpu.SemaphoreType.DMA((3,)),
            pltpu.SemaphoreType.DMA((count,)),
            pltpu.SemaphoreType.DMA((1,)),
            pltpu.SemaphoreType.DMA((max(count - 1, 1), share // chunk)),
            pltpu.SemaphoreType.DMA((2,)),
        ],
        compiler_params=pltpu.CompilerParams(
            collective_id=0, has_side_effects=True, vmem_limit_bytes=36 * 1024 * 1024
        ),
        name="absorb_exchange_gauge",
    )(
        pltpu.with_memory_space_constraint(environment.reshape(count, rows, w, w, legs), pltpu.HBM),
        pltpu.with_memory_space_constraint(peps.reshape(4, w ** 3, w), pltpu.HBM),
        pltpu.with_memory_space_constraint(operators, pltpu.HBM),
        pltpu.with_memory_space_constraint(gauge, pltpu.HBM),
    )
    return scaled(gauged, sums, chi * square * legs)


def solution(mesh):
    placed = (P(None, "bits", None, None), P(), P(), P())
    return jax.shard_map(
        body, mesh=mesh, in_specs=placed, out_specs=(P(None, None, "bits"), P()), check_vma=False
    )
```
